256 devices in a mesh: expert: 16 (over y, x), dp: 16 (over z, core).
Axes of the slice: x: 4, y: 4, z: 8, core: 2. Of those that a mesh axis runs over, the one named last changes fastest.
Arguments:
- acts: bfloat16 [256, 16, 16, 3584], P(('expert', 'dp')), may hold values from -6 to 6
- grad_out: bfloat16 [256, 16, 16, 1024], P(('expert', 'dp')), may hold values from -0.125 to 0.125
- routing_counts: int32 [256, 16], P(('expert', 'dp')), may hold values from 1 to 16, as said below
- left_basis: bfloat16 [16, 3584, 3584], P('expert', 'dp'), may hold values from -1 to 1, as said below
- right_basis: bfloat16 [16, 1024, 1024], P('expert'), may hold values from -1 to 1, as said below
- first_moment: float32 [16, 3584, 1024], P('expert', 'dp'), may hold values from -3 to 3
- second_moment: float32 [16, 3584, 1024], P('expert', 'dp'), may hold values from 0.05 to 2000
Outputs:
- step_delta: bfloat16 [16, 3584, 1024], P('expert', 'dp')
- first_out: float32 [16, 3584, 1024], P('expert', 'dp')
- second_out: float32 [16, 3584, 1024], P('expert', 'dp')
- expert_rms: float32 [16], P('expert')
The draws below stay inside these ranges and needn't reach their ends.
Inputs may be any that keep to these rules, and one draw needn't show every extreme that they name: Slot s of shard i for expert e carries a routed token when s < routing_counts[i, e]; the other slots hold leftover values that belong to no token. In every shard some expert has all 16 slots live. `left_basis`: each expert's block is an orthogonal matrix rounded to bfloat16. `right_basis`: each expert's block is an orthogonal matrix rounded to bfloat16.
All inputs are finite; a program needn't handle non-finite values.
Results may differ from the reference program's by a relative error of at most 0.013.
Values may be sent and summed in bfloat16 or wider, within the bound.
A program may use at most 64 MiB of HBM per device.

```python
import jax
import jax.numpy as jnp
from jax import lax

D = 3584
FF = 1024
CAP = 16
EXPERTS = 16
SHARDS = 256
N_EXPERT = 16
N_DP = 16


def orthogonal_blocks(base_key, block_count, order, diagonal_weight):

    def single(block_key):
        normal_block = jax.random.normal(block_key, (order, order), jnp.float32) / jnp.sqrt(jnp.float32(order))
        normal_block = normal_block + diagonal_weight * jnp.eye(order, dtype=jnp.float32)
        orthonormal, triangle = jnp.linalg.qr(normal_block)
        return orthonormal * jnp.sign(jnp.diagonal(triangle))[None, :]
    return lax.map(single, jax.random.split(base_key, block_count))


def draw_left_basis(key, part):
    return orthogonal_blocks(jax.random.fold_in(key, 11), EXPERTS, D, 1.5).astype(jnp.bfloat16)


def draw_right_basis(key, part):
    return orthogonal_blocks(jax.random.fold_in(key, 23), EXPERTS, FF, 0.0).astype(jnp.bfloat16)


def draw_second_moment(key, part):
    base_key = jax.random.fold_in(key, 37)
    log_low = jnp.log(jnp.float32(0.05))
    log_high = jnp.log(jnp.float32(2.0))
    base = jnp.exp(jax.random.uniform(base_key, (EXPERTS, D, FF), jnp.float32, log_low, log_high))
    row_span = 16.0
    expert_span = 9.0
    row_place = lax.broadcasted_iota(jnp.float32, (EXPERTS, D, FF), 1) / D
    expert_place = lax.broadcasted_iota(jnp.float32, (EXPERTS, D, FF), 0) / EXPERTS
    row_factor = jnp.exp((1.0 - row_place) * jnp.log(jnp.float32(row_span)))
    expert_factor = jnp.exp((1.0 - expert_place) * jnp.log(jnp.float32(expert_span)))
    return (base * row_factor * expert_factor).astype(jnp.float32)


def draw_routing_counts(key, part):
    first_key, second_key = jax.random.split(jax.random.fold_in(key, 5))
    counts = jax.random.randint(first_key, (SHARDS, EXPERTS), 1, CAP + 1)
    filled = jax.random.randint(second_key, (SHARDS, 1), 0, EXPERTS)
    column = lax.broadcasted_iota(jnp.int32, (SHARDS, EXPERTS), 1)
    return jnp.where(column == filled, CAP, counts).astype(jnp.int32)


def level_of(rng, shape, pieces, low, high):
    def one(position, parts):
        steps = jax.random.uniform(jax.random.fold_in(jax.random.fold_in(rng, 6), position), (parts,), jnp.float32, low / len(pieces), high / len(pieces))
        return jnp.repeat(jnp.exp(steps), shape[position] // parts).reshape((-1,) + (1,) * (len(shape) - position - 1))

    loudness = one(*pieces[0])
    for cut in pieces[1:]:
        loudness = loudness * one(*cut)
    return loudness


def centred(rng, extent, scale, bound, shards=(), held_as=jnp.bfloat16):
    values = jax.random.normal(rng, extent, jnp.float32) * scale
    if len(shards) > 0:
        values = level_of(rng, extent, shards, -0.22, 0.18) * values
    return jnp.clip(values, min=-bound, max=bound).astype(held_as)


def setup_inputs(seed: int = 0) -> dict:
    keys = jax.random.split(jax.random.key(seed), 8)
    return {
        "acts": centred(keys[0], (SHARDS, EXPERTS, CAP, D), 1.0, 6.0, ((0, 256),)),
        "grad_out": centred(keys[1], (SHARDS, EXPERTS, CAP, FF), (CAP * SHARDS // 2) ** -0.5, 0.125, ((0, 256),)),
        "routing_counts": draw_routing_counts(jax.random.fold_in(keys[7], 71), 0),
        "left_basis": draw_left_basis(jax.random.fold_in(keys[7], 71), 0),
        "right_basis": draw_right_basis(jax.random.fold_in(keys[7], 71), 0),
        "first_moment": centred(keys[5], (EXPERTS, D, FF), 0.5, 3.0, ((0, 16), (1, 16)), jnp.float32),
        "second_moment": draw_second_moment(jax.random.fold_in(keys[7], 71), 0),
    }


BETA_ONE = 0.9
BETA_TWO = 0.95
EPS_DIVIDE = 1e-08
EPS_MEAN = 1e-06

def reference(acts, grad_out, routing_counts, left_basis, right_basis, first_moment, second_moment):
    slot_index = lax.broadcasted_iota(jnp.int32, (SHARDS, EXPERTS, CAP), 2)
    live_slots = (slot_index < routing_counts[:, :, None])[..., None]
    acts_live = jnp.where(live_slots, acts, jnp.zeros((), jnp.bfloat16))
    grads_live = jnp.where(live_slots, grad_out, jnp.zeros((), jnp.bfloat16))
    acts_split = acts_live.reshape(N_EXPERT, N_DP, EXPERTS, CAP, D)
    grads_split = grads_live.reshape(N_EXPERT, N_DP, EXPERTS, CAP, FF)

    def one_expert(expert_index):
        token_acts = lax.dynamic_index_in_dim(acts_split, expert_index, 2, keepdims=False)
        token_grads = lax.dynamic_index_in_dim(grads_split, expert_index, 2, keepdims=False)
        token_acts = jnp.swapaxes(token_acts, 0, 1).reshape(N_DP, N_EXPERT * CAP, D)
        token_grads = jnp.swapaxes(token_grads, 0, 1).reshape(N_DP, N_EXPERT * CAP, FF)

        def add_partial(running, operand_pair):
            partial_value = jnp.dot(operand_pair[0].T.astype(jnp.float32), operand_pair[1].astype(jnp.float32), preferred_element_type=jnp.float32)
            partial_value = lax.optimization_barrier(partial_value.astype(jnp.bfloat16))
            return (running + partial_value.astype(jnp.float32), None)
        summed, _ = lax.scan(add_partial, jnp.zeros((D, FF), jnp.float32), (token_acts, token_grads))
        gradient = summed.astype(jnp.bfloat16)
        left_block = lax.dynamic_index_in_dim(left_basis, expert_index, 0, keepdims=False)
        right_block = lax.dynamic_index_in_dim(right_basis, expert_index, 0, keepdims=False)
        first_block = lax.dynamic_index_in_dim(first_moment, expert_index, 0, keepdims=False)
        second_block = lax.dynamic_index_in_dim(second_moment, expert_index, 0, keepdims=False)
        right_turned = jnp.dot(gradient.astype(jnp.float32), right_block.astype(jnp.float32), preferred_element_type=jnp.float32).astype(jnp.bfloat16)
        rotated = jnp.dot(left_block.T.astype(jnp.float32), right_turned.astype(jnp.float32), preferred_element_type=jnp.float32)
        first_new = BETA_ONE * first_block + (1.0 - BETA_ONE) * rotated
        second_new = BETA_TWO * second_block + (1.0 - BETA_TWO) * rotated * rotated
        direction = (first_new / (jnp.sqrt(second_new) + EPS_DIVIDE)).astype(jnp.bfloat16)
        restored = jnp.dot(direction.astype(jnp.float32), right_block.T.astype(jnp.float32), preferred_element_type=jnp.float32).astype(jnp.bfloat16)
        update = jnp.dot(left_block.astype(jnp.float32), restored.astype(jnp.float32), preferred_element_type=jnp.float32)
        squares = jnp.sum(update * update)
        return (update, first_new, second_new, squares)
    updates, first_out, second_out, squares = lax.map(one_expert, jnp.arange(EXPERTS, dtype=jnp.int32))
    expert_rms = jnp.sqrt(squares / (D * FF) + EPS_MEAN)
    mean_norm = jnp.mean(expert_rms)
    step_delta = (-updates / jnp.maximum(expert_rms, mean_norm)[:, None, None]).astype(jnp.bfloat16)
    return (step_delta, first_out, second_out, expert_rms)
```

```python
import functools

import jax
import jax.numpy as jnp
from jax import lax
from jax.experimental import pallas as pl
from jax.experimental.pallas import tpu as pltpu
from jax.sharding import Mesh
from jax.sharding import PartitionSpec as P

AXES = ("y", "x", "z", "core")
EXPERT = ("y", "x")
DP = ("z", "core")
NY, NX, NZ, NC = 4, 4, 8, 2
MESH = pl.DeviceIdType.MESH

BETA_ONE = 0.9
BETA_TWO = 0.95
EPS_DIVIDE = 1e-08
EPS_MEAN = 1e-06

PLANE = (
    (0, 1), (1, 0), (0, 3), (3, 0), (1, 1), (3, 3), (1, 3), (3, 1),
    (2, 0), (0, 2), (1, 2), (2, 1), (3, 2), (2, 3), (2, 2),
)
COLUMN = tuple((dz, dc) for dz in range(NZ) for dc in range(NC) if dz or dc)
REDUCE = ((4, 0), (3, 1), (3, 0), (2, 1), (2, 0), (1, 1), (1, 0))
ADDS = (None, None, 0, 1, 2, 3, 4)
GATHER = ((0, 0), (0, 1), (1, 0), (1, 1), (2, 0), (2, 1), (3, 0))


def kernel(
    counts, acts, grads, left, right, first_in, second_in,
    delta_out, first_out, second_out, rms_out,
    a_all, g_own, g_all, l_all, r_all, m1, m2, g_turned, part, s_one, v_one, s_two, v_two,
    turned, rot, rot_send, res_send, x_all, upd, upd_other, d_buf, f_buf, s_buf,
    n_col, n_exp,
    load_sem, a_send, a_recv, g_send, g_recv, fwd_send, fwd_recv, pair_send, pair_recv,
    r_send, r_recv, x_send, x_recv, n_send, n_recv, out_sem,
):
    y, x, z, c = (lax.axis_index(a) for a in AXES)
    other = 1 - c
    rows = left.shape[0]
    block = 2 * rows
    width = left.shape[1]
    hidden = grads.shape[1]
    half = hidden // 2
    quarter = half // 2
    slots = acts.shape[0] // (NY * NX)
    tokens = NY * NX * slots
    pair_wide = 2 * block

    def mod(v, n):
        return lax.rem(v + n, n)

    partner = (y, x, z, other)
    plane = [(mod(y + dy, NY), mod(x + dx, NX), z, c) for dy, dx in PLANE]
    column = [(y, x, mod(z + dz, NZ), mod(c + dc, NC)) for dz, dc in COLUMN]
    up = (y, x, mod(z + 1, NZ), c)
    down = (y, x, mod(z - 1, NZ), c)

    def remote(src, dst, send, recv, device):
        return pltpu.make_async_remote_copy(
            src_ref=src, dst_ref=dst, send_sem=send, recv_sem=recv, device_id=device, device_id_type=MESH
        )

    barrier = pltpu.get_barrier_semaphore()
    for device in plane + column:
        pl.semaphore_signal(barrier, 1, device_id=device, device_id_type=MESH)

    own_expert = y * NX + x
    mine_l = pl.ds(pl.multiple_of(c * rows, rows), rows)
    load_g = pltpu.make_async_copy(grads, g_own, load_sem.at[0])
    load_a = pltpu.make_async_copy(
        acts.at[pl.ds(pl.multiple_of(own_expert * slots, slots), slots), :],
        a_all.at[pl.ds(pl.multiple_of(c * tokens, tokens), slots), :],
        load_sem.at[1],
    )
    load_l = pltpu.make_async_copy(left, l_all.at[mine_l, :], load_sem.at[2])
    load_r = pltpu.make_async_copy(right, r_all, load_sem.at[3])
    load_m1 = pltpu.make_async_copy(first_in, m1, load_sem.at[4])
    load_m2 = pltpu.make_async_copy(second_in, m2, load_sem.at[5])
    for load in (load_g, load_a, load_l, load_r, load_m1, load_m2):
        load.start()
    load_g.wait()
    slot_index = lax.broadcasted_iota(jnp.int32, (slots, hidden), 0)
    for e in range(NY * NX):
        here = slice(e * slots, (e + 1) * slots)
        g_own[here, :] = jnp.where(slot_index < counts[0, e], g_own[here, :].astype(jnp.float32), 0.0).astype(jnp.bfloat16)
    pl.semaphore_wait(barrier, len(plane) + len(column))

    def token_rows(core, i):
        return pl.ds(pl.multiple_of(core * tokens + i * slots, slots), slots)

    g_copies, a_copies = [], []
    for i, ((dy, dx), device) in enumerate(zip(PLANE, plane)):
        expert = device[0] * NX + device[1]
        src = pl.ds(pl.multiple_of(expert * slots, slots), slots)
        dst = token_rows(c, i + 1)
        g_copies.append(remote(g_own.at[src, :], g_all.at[dst, :], g_send.at[i], g_recv.at[i], device))
        a_copies.append(remote(acts.at[src, :], a_all.at[dst, :], a_send.at[i], a_recv.at[i], device))
    for copy in g_copies:
        copy.start()
    for copy in a_copies:
        copy.start()
    own_g = pl.ds(pl.multiple_of(own_expert * slots, slots), slots)
    g_all[token_rows(c, 0), :] = g_own[own_g, :]
    load_a.wait()
    load_l.wait()
    l_copy = remote(l_all.at[mine_l, :], l_all.at[mine_l, :], pair_send.at[0], pair_recv.at[0], partner)
    l_copy.start()
    forwards = []
    for i in range(NY * NX):
        here = token_rows(c, i)
        forwards.append(remote(g_all.at[here, :], g_all.at[here, :], fwd_send.at[i], fwd_recv.at[0], partner))
        if i:
            g_copies[i - 1].wait_recv()
        forwards[-1].start()
    load_r.wait()
    load_m1.wait()
    load_m2.wait()
    for i in range(NY * NX):
        here = token_rows(c, i)
        forwards.append(remote(a_all.at[here, :], a_all.at[here, :], fwd_send.at[NY * NX + i], fwd_recv.at[1], partner))
        if i:
            a_copies[i - 1].wait_recv()
        forwards[-1].start()
    theirs = pl.ds(pl.multiple_of(other * tokens, tokens), tokens)
    remote(g_all.at[theirs, :], g_all.at[theirs, :], fwd_send.at[0], fwd_recv.at[0], partner).wait_recv()
    g_turned[...] = jnp.dot(
        g_all[...], r_all[:, pl.ds(pl.multiple_of(c * half, half), half)], preferred_element_type=jnp.float32
    ).astype(jnp.bfloat16)
    remote(a_all.at[theirs, :], a_all.at[theirs, :], fwd_send.at[0], fwd_recv.at[1], partner).wait_recv()
    l_copy.wait_recv()

    def reduce(lhs, rhs, send_buf, recv_buf, sems, finish):
        copies = []
        for k, (away, part_of) in enumerate(REDUCE):
            ways = []
            for way, device in ((0, up), (1, down)):
                ways.append(
                    remote(
                        send_buf.at[way, k], recv_buf.at[way, k],
                        r_send.at[sems, way, k], r_recv.at[sems, way, k], device,
                    )
                )
            copies.append(ways)

        def rows_of(away, way):
            owner = mod(z + away, NZ) if way == 0 else mod(z - away, NZ)
            return pl.multiple_of(owner * block, block)

        chunk = block // 4

        def send(k):
            away, part_of = REDUCE[k]
            for way in range(2):
                cols = slice((part_of ^ way) * quarter, ((part_of ^ way) + 1) * quarter)
                start = rows_of(away, way)
                if ADDS[k] is not None:
                    copies[ADDS[k]][way].wait_recv()

                def one(t, _):
                    at = pl.multiple_of(t * chunk, chunk)
                    value = part[pl.ds(start + at, chunk), cols]
                    if ADDS[k] is not None:
                        value = value + recv_buf[way, ADDS[k], pl.ds(at, chunk), :].astype(jnp.float32)
                    send_buf[way, k, pl.ds(at, chunk), :] = value.astype(jnp.bfloat16)
                    return 0

                lax.fori_loop(0, 4, one, 0)
                copies[k][way].start()

        def one_pair(i, _):
            which = lax.rem(z // 2 + 2 + i, NZ // 2)
            at = pl.multiple_of(which * pair_wide, pair_wide)
            part[pl.ds(at, pair_wide), :] = lax.dot_general(
                lhs[:, pl.ds(at, pair_wide)], rhs[...], (((0,), (0,)), ((), ())), preferred_element_type=jnp.float32
            )

            @pl.when(i == 0)
            def _():
                send(0)

            return 0

        lax.fori_loop(0, NZ // 2, one_pair, 0)
        for k in range(1, len(REDUCE)):
            send(k)
        own = pl.multiple_of(z * block, block)
        for k in (len(REDUCE) - 2, len(REDUCE) - 1):
            for way in range(2):
                copies[k][way].wait_recv()
        last, before = len(REDUCE) - 1, len(REDUCE) - 2

        def close(t, _):
            at = pl.multiple_of(t * chunk, chunk)
            for q in range(2):
                up_k, down_k = (last, before) if q == 0 else (before, last)
                value = (
                    part[pl.ds(own + at, chunk), q * quarter : (q + 1) * quarter]
                    + recv_buf[0, up_k, pl.ds(at, chunk), :].astype(jnp.float32)
                    + recv_buf[1, down_k, pl.ds(at, chunk), :].astype(jnp.float32)
                )
                finish(at, chunk, q, value)
            return 0

        lax.fori_loop(0, 4, close, 0)
        return copies

    def keep_turned(at, chunk, q, value):
        turned[pl.ds(at, chunk), q * quarter : (q + 1) * quarter] = value.astype(jnp.bfloat16)

    def keep_rotated(at, chunk, q, value):
        rot_send[pl.ds(at, chunk), q * quarter : (q + 1) * quarter] = value

    copies_one = reduce(a_all, g_turned, s_one, v_one, 0, keep_turned)
    copies_two = reduce(l_all, turned, s_two, v_two, 1, keep_rotated)

    theirs_l = pl.ds(pl.multiple_of(other * rows, rows), rows)
    rot_copy = remote(rot_send.at[theirs_l, :], rot.at[c], pair_send.at[1], pair_recv.at[1], partner)
    rot_copy.start()
    rot[c] = rot_send[mine_l, :]
    rot_copy.wait_recv()
    for h in range(2):
        cols = slice(h * half, (h + 1) * half)
        turned_back = rot[h]
        first = BETA_ONE * m1[:, cols] + (1.0 - BETA_ONE) * turned_back
        second = BETA_TWO * m2[:, cols] + (1.0 - BETA_TWO) * turned_back * turned_back
        f_buf[:, cols] = first
        s_buf[:, cols] = second
        d_buf[:, cols] = (first / (jnp.sqrt(second) + EPS_DIVIDE)).astype(jnp.bfloat16)
    out_first = pltpu.make_async_copy(f_buf, first_out, out_sem.at[0])
    out_second = pltpu.make_async_copy(s_buf, second_out, out_sem.at[1])
    out_first.start()
    out_second.start()

    def restore(which):
        return lax.dot_general(
            d_buf[...], r_all[pl.ds(pl.multiple_of(which * half, half), half), :],
            (((1,), (1,)), ((), ())), preferred_element_type=jnp.float32,
        ).astype(jnp.bfloat16)

    def gather_rows(back, way, part_of):
        owner = mod(z - back, NZ) if way == 0 else mod(z + back, NZ)
        core = c if part_of ^ way == 0 else other
        return pl.ds(pl.multiple_of(owner * block + core * rows, rows), rows)

    res_send[...] = restore(other)
    res_copy = remote(res_send, x_all.at[gather_rows(0, 0, 0), :], pair_send.at[2], pair_recv.at[2], partner)
    res_copy.start()
    x_all[gather_rows(0, 0, 0), :] = restore(c)

    x_copies = []
    for k, (back, part_of) in enumerate(GATHER):
        ways = []
        for way, device in ((0, up), (1, down)):
            here = gather_rows(back, way, part_of)
            ways.append(remote(x_all.at[here, :], x_all.at[here, :], x_send.at[way, k], x_recv.at[way, k], device))
        x_copies.append(ways)

    def update_pair(i):
        which = lax.rem(z // 2 + i, NZ // 2)
        at = pl.multiple_of(which * pair_wide, pair_wide)
        return jnp.dot(l_all[:, pl.ds(at, pair_wide)], x_all[pl.ds(at, pair_wide), :], preferred_element_type=jnp.float32)

    x_copies[0][0].start()
    res_copy.wait_recv()
    x_copies[0][1].start()
    for way in range(2):
        x_copies[1][way].start()
    for k in range(2, len(GATHER)):
        for way in range(2):
            x_copies[k - 2][way].wait_recv()
            x_copies[k][way].start()
        if k == 3:
            upd[...] = update_pair(0)
    odd = lax.rem(z, 2)
    upd[...] += update_pair(3 - 2 * odd)
    for way in range(2):
        x_copies[5][way].wait_recv()
    upd[...] += update_pair(1 + 2 * odd)
    for way in range(2):
        x_copies[6][way].wait_recv()
    upd[...] += update_pair(2)

    squares = jnp.sum(upd[...] * upd[...])
    n_col[0] = jnp.broadcast_to(squares, n_col.shape[1:])
    upd_copy = remote(upd.at[theirs_l, :], upd_other, pair_send.at[3], pair_recv.at[3], partner)
    n_copies = [
        remote(n_col.at[0], n_col.at[1 + i], n_send.at[0, i], n_recv.at[0], device) for i, device in enumerate(column)
    ]
    for copy in n_copies:
        copy.start()
    upd_copy.start()
    remote(n_col.at[1:], n_col.at[1:], n_send.at[0, 0], n_recv.at[0], partner).wait_recv()
    total = jnp.zeros(n_col.shape[1:], jnp.float32)
    for d in range(NZ * NC):
        back_z = lax.rem(z - d // NC + NZ, NZ)
        back_c = lax.rem(c - d % NC + NC, NC)
        total = total + n_col[back_z * NC + back_c]
    n_exp[0] = total
    e_copies = [
        remote(n_exp.at[0], n_exp.at[1 + i], n_send.at[1, i], n_recv.at[1], device) for i, device in enumerate(plane)
    ]
    for copy in e_copies:
        copy.start()
    upd_copy.wait_recv()
    remote(n_exp.at[1:], n_exp.at[1:], n_send.at[1, 0], n_recv.at[1], partner).wait_recv()
    cells = float(width * hidden)
    own_norm = jnp.sqrt(total / cells + EPS_MEAN)
    norms = jnp.zeros_like(total)
    for e in range(NY * NX):
        norms = norms + jnp.sqrt(n_exp[e] / cells + EPS_MEAN)
    below = jnp.maximum(own_norm, norms / float(NY * NX))
    rms_out[...] = own_norm
    below = below[0:1, 0:1]
    own_half = upd[mine_l, :]
    other_half = upd_other[...]
    low = jnp.where(c == 0, own_half, other_half)
    high = jnp.where(c == 0, other_half, own_half)
    delta_out[:, :half] = (-low / below).astype(jnp.bfloat16)
    delta_out[:, half:] = (-high / below).astype(jnp.bfloat16)

    for copy in g_copies + a_copies + forwards + [l_copy, rot_copy, res_copy, upd_copy] + n_copies + e_copies:
        copy.wait_send()
    for ways in copies_one + copies_two + x_copies:
        for copy in ways:
            copy.wait_send()
    out_first.wait()
    out_second.wait()


def local(acts, grad_out, routing_counts, left_basis, right_basis, first_moment, second_moment):
    width, hidden = acts.shape[-1], grad_out.shape[-1]
    rows = left_basis.shape[1]
    block, half = 2 * rows, hidden // 2
    quarter = half // 2
    own_tokens = acts.shape[1] * acts.shape[2]
    both = 2 * own_tokens
    bf16, f32 = jnp.bfloat16, jnp.float32
    vmem, dma = pltpu.VMEM, pltpu.SemaphoreType.DMA
    hbm = pl.BlockSpec(memory_space=pl.ANY)
    whole = pl.BlockSpec(memory_space=pltpu.VMEM)
    messages = len(REDUCE)
    delta, first, second, rms = pl.pallas_call(
        kernel,
        name="soap_step",
        out_shape=(
            jax.ShapeDtypeStruct((rows, hidden), bf16),
            jax.ShapeDtypeStruct((rows, hidden), f32),
            jax.ShapeDtypeStruct((rows, hidden), f32),
            jax.ShapeDtypeStruct((8, 128), f32),
        ),
        in_specs=[pl.BlockSpec(memory_space=pltpu.SMEM)] + [hbm] * 6,
        out_specs=(whole, hbm, hbm, whole),
        scratch_shapes=[
            vmem((both, width), bf16),
            vmem((own_tokens, hidden), bf16),
            vmem((both, hidden), bf16),
            vmem((block, width), bf16),
            vmem((hidden, hidden), bf16),
            vmem((rows, hidden), f32),
            vmem((rows, hidden), f32),
            vmem((both, half), bf16),
            vmem((width, half), f32),
            vmem((2, messages, block, quarter), bf16),
            vmem((2, messages, block, quarter), bf16),
            vmem((2, messages, block, quarter), bf16),
            vmem((2, messages, block, quarter), bf16),
            vmem((block, half), bf16),
            vmem((2, rows, half), f32),
            vmem((block, half), f32),
            vmem((rows, half), bf16),
            vmem((width, half), bf16),
            vmem((block, half), f32),
            vmem((rows, half), f32),
            vmem((rows, hidden), bf16),
            vmem((rows, hidden), f32),
            vmem((rows, hidden), f32),
            vmem((NZ * NC, 8, 128), f32),
            vmem((NY * NX, 8, 128), f32),
            dma((6,)),
            dma((15,)), dma((15,)), dma((15,)), dma((15,)),
            dma((32,)), dma((2,)),
            dma((4,)), dma((4,)),
            dma((2, 2, messages)), dma((2, 2, messages)),
            dma((2, messages)), dma((2, messages)),
            dma((2, 15)), dma((2,)),
            dma((2,)),
        ],
        compiler_params=pltpu.CompilerParams(
            collective_id=0, has_side_effects=True, vmem_limit_bytes=64 * 1024 * 1024 - 128 * 1024
        ),
    )(
        routing_counts,
        acts.reshape(own_tokens, width),
        grad_out.reshape(own_tokens, hidden),
        left_basis[0],
        right_basis[0],
        first_moment[0],
        second_moment[0],
    )
    return delta[None], first[None], second[None], rms[0, :1]


def solution(mesh):
    split = Mesh(mesh.devices.reshape(NY, NX, NZ, NC), AXES)
    placed = (
        P(AXES, None, None, None),
        P(AXES, None, None, None),
        P(AXES, None),
        P(EXPERT, DP, None),
        P(EXPERT, None, None),
        P(EXPERT, DP, None),
        P(EXPERT, DP, None),
    )
    return jax.shard_map(
        local,
        mesh=split,
        in_specs=placed,
        out_specs=(P(EXPERT, DP, None), P(EXPERT, DP, None), P(EXPERT, DP, None), P(EXPERT)),
        check_vma=False,
    )
```

```python
import functools

import jax
import jax.numpy as jnp
from jax import lax
from jax.experimental import pallas as pl
from jax.experimental.pallas import tpu as pltpu
from jax.sharding import Mesh
from jax.sharding import PartitionSpec as P

AXES = ("y", "x", "z", "core")
EXPERT = ("y", "x")
DP = ("z", "core")
NY, NX, NZ, NC = 4, 4, 8, 2
MESH = pl.DeviceIdType.MESH

BETA_ONE = 0.9
BETA_TWO = 0.95
EPS_DIVIDE = 1e-08
EPS_MEAN = 1e-06

PLANE = (
    (0, 1), (1, 0), (0, 3), (3, 0), (1, 1), (3, 3), (1, 3), (3, 1),
    (2, 0), (0, 2), (1, 2), (2, 1), (3, 2), (2, 3), (2, 2),
)
COLUMN = tuple((dz, dc) for dz in range(NZ) for dc in range(NC) if dz or dc)
ONE_UP = (
    (4, 0, 0), (4, 1, 1), (3, 1, 0), (3, 0, 1), (3, 0, 0), (3, 1, 1), (2, 1, 0),
    (2, 0, 0), (2, 0, 1), (1, 1, 0), (1, 0, 0), (2, 1, 1), (1, 0, 1), (1, 1, 1),
)
ONE = (ONE_UP, tuple((away, 1 - r, q) for away, r, q in ONE_UP))
TWO = (
    (
        (4, 0, 0), (3, 1, 0), (4, 1, 1), (3, 0, 1), (3, 0, 0), (2, 1, 0), (3, 1, 1),
        (2, 0, 1), (2, 0, 0), (1, 0, 1), (1, 0, 0), (2, 1, 1), (1, 1, 0), (1, 1, 1),
    ),
    (
        (4, 1, 0), (3, 0, 0), (4, 0, 1), (3, 1, 1), (3, 1, 0), (2, 0, 0), (3, 0, 1),
        (2, 1, 1), (2, 0, 1), (1, 0, 0), (1, 0, 1), (2, 1, 0), (1, 1, 1), (1, 1, 0),
    ),
)
NEAR = tuple((back, r, q) for back in range(3) for r in range(2) for q in range(2))
GATHER = (NEAR + ((3, 0, 0), (3, 0, 1)), NEAR + ((3, 1, 0), (3, 1, 1)))
MESSAGES = len(ONE_UP)


def before(table, message):
    away, r, q = message
    return {m: k for k, m in enumerate(table)}.get((away + 1, r, q))


def kernel(
    counts_in, acts, grads, left, right, first_in, second_in,
    delta_out, first_out, second_out, rms_out,
    counts, a_all, g_own, g_all, l_all, l_turn, r_all, m1, m2, g_turned, part, s_one, v_one, s_two, v_two,
    turned, rot_own, rot_in, res_send, x_all, upd, upd_other, d_buf, f_buf, s_buf, n_col, n_exp,
    load_sem, t_send, t_recv, fwd_send, fwd_recv, pair_send, pair_recv,
    r_send, r_recv, x_send, x_recv, n_send, n_recv, out_sem,
):
    y, x, z, c = (lax.axis_index(a) for a in AXES)
    other = 1 - c
    rows = left.shape[0]
    block = 2 * rows
    width = left.shape[1]
    hidden = grads.shape[1]
    half = hidden // 2
    quarter = half // 2
    slots = acts.shape[0] // (NY * NX)
    tokens = NY * NX * slots
    pair_wide = 2 * block

    def mod(v, n):
        return lax.rem(v + n, n)

    partner = (y, x, z, other)
    plane = [(mod(y + dy, NY), mod(x + dx, NX), z, c) for dy, dx in PLANE]
    column = [(y, x, mod(z + dz, NZ), mod(c + dc, NC)) for dz, dc in COLUMN]
    up = (y, x, mod(z + 1, NZ), c)
    down = (y, x, mod(z - 1, NZ), c)

    def remote(src, dst, send, recv, device):
        return pltpu.make_async_remote_copy(
            src_ref=src, dst_ref=dst, send_sem=send, recv_sem=recv, device_id=device, device_id_type=MESH
        )

    barrier = pltpu.get_barrier_semaphore()
    for device in plane + column:
        pl.semaphore_signal(barrier, 1, device_id=device, device_id_type=MESH)

    own_expert = y * NX + x
    mine_l = pl.ds(pl.multiple_of(c * rows, rows), rows)
    load_c = pltpu.make_async_copy(counts_in, counts, load_sem.at[6])
    load_g = pltpu.make_async_copy(grads, g_own, load_sem.at[0])
    load_a = pltpu.make_async_copy(
        acts.at[pl.ds(pl.multiple_of(own_expert * slots, slots), slots), :],
        a_all.at[pl.ds(pl.multiple_of(c * tokens, tokens), slots), :],
        load_sem.at[1],
    )
    load_l = pltpu.make_async_copy(left, l_all.at[mine_l, :], load_sem.at[2])
    load_r = pltpu.make_async_copy(right, r_all, load_sem.at[3])
    load_m1 = pltpu.make_async_copy(first_in, m1, load_sem.at[4])
    load_m2 = pltpu.make_async_copy(second_in, m2, load_sem.at[5])
    load_c.start()
    load_g.start()
    load_l.start()
    load_c.wait()
    load_g.wait()
    for load in (load_a, load_r, load_m1, load_m2):
        load.start()
    slot_index = lax.broadcasted_iota(jnp.int32, (slots, hidden), 0)
    for e in range(NY * NX):
        here = slice(e * slots, (e + 1) * slots)
        g_own[here, :] = jnp.where(slot_index < counts[0, e], g_own[here, :].astype(jnp.float32), 0.0).astype(jnp.bfloat16)
    pl.semaphore_wait(barrier, len(plane) + len(column))

    odd = lax.rem(z, 2)
    pair_of = [
        lax.rem(z // 2 + i, NZ // 2) * pair_wide for i in (2, 1 + 2 * odd, 3 - 2 * odd, 0)
    ]
    pairs = [pl.ds(pl.multiple_of(at, pair_wide), pair_wide) for at in pair_of]
    wide, rest = pair_wide * 4 // 7, pair_wide * 3 // 7

    def window(at, size):
        return pl.ds(pl.multiple_of(at, pair_wide // 7), size)

    groups = [None]
    for one, two in ((0, 1), (2, 3)):
        groups += [
            window(pair_of[one] + rest * odd, wide),
            window(pair_of[two] + rest * (1 - odd), wide),
            window(pair_of[one] + wide * (1 - odd), rest),
            window(pair_of[two] + wide * odd, rest),
        ]

    def token_rows(core, i):
        return pl.ds(pl.multiple_of(core * tokens + i * slots, slots), slots)

    t_copies = []
    for g, cols in enumerate(groups):
        copies = []
        for i, device in enumerate(plane):
            expert = device[0] * NX + device[1]
            src = pl.ds(pl.multiple_of(expert * slots, slots), slots)
            dst = token_rows(c, i + 1)
            if g == 0:
                ends = g_own.at[src, :], g_all.at[dst, :]
            else:
                ends = acts.at[src, cols], a_all.at[dst, cols]
            copies.append(remote(*ends, t_send.at[g], t_recv.at[g], device))
        t_copies.append(copies)

    def token_start(g):
        for copy in t_copies[g]:
            copy.start()

    def group_of(g, core, first, count):
        here = pl.ds(pl.multiple_of(core * tokens + first, slots), count)
        return g_all.at[here, :] if g == 0 else a_all.at[here, groups[g]]

    def token_wait(g):
        arrived = group_of(g, c, slots, tokens - slots)
        return remote(arrived, arrived, t_send.at[g], t_recv.at[g], partner)

    forwards = []
    for g in range(len(groups)):
        mine = group_of(g, c, 0, tokens)
        forwards.append(remote(mine, mine, fwd_send.at[g], fwd_recv.at[g], partner))

    def token_finish(g):
        token_wait(g).wait_recv()
        forwards[g].start()
        if g + 3 < len(groups):
            token_wait(g).wait_send()
            token_start(g + 3)
        theirs = group_of(g, other, 0, tokens)
        remote(theirs, theirs, fwd_send.at[g], fwd_recv.at[g], partner).wait_recv()

    for g in range(3):
        token_start(g)
    own_g = pl.ds(pl.multiple_of(own_expert * slots, slots), slots)
    g_all[token_rows(c, 0), :] = g_own[own_g, :]
    load_l.wait()
    l_copy = remote(l_all.at[mine_l, :], l_all.at[mine_l, :], pair_send.at[0], pair_recv.at[0], partner)
    l_copy.start()
    load_a.wait()
    load_r.wait()
    load_m1.wait()
    load_m2.wait()
    l_copy.wait_recv()
    for p in range(NZ // 2):
        at = slice(p * pair_wide, (p + 1) * pair_wide)
        l_turn[at, :] = l_all[:, at].T
    token_finish(0)
    g_turned[...] = jnp.dot(
        g_all[...], r_all[:, pl.ds(pl.multiple_of(c * half, half), half)], preferred_element_type=jnp.float32
    ).astype(jnp.bfloat16)

    chunk = rows // 2

    def message(tables, send_buf, recv_buf, sems, k, way):
        return remote(
            send_buf.at[way, k], recv_buf.at[way, k], r_send.at[sems, way, k], r_recv.at[sems, way, k], (up, down)[way]
        )

    def send(tables, send_buf, recv_buf, sems, k):
        for way in range(2):
            away, r, q = tables[way][k]
            owner = mod(z + away, NZ) if way == 0 else mod(z - away, NZ)
            start = owner * block + r * rows
            added = before(tables[way], tables[way][k])
            if added is not None:
                message(tables, send_buf, recv_buf, sems, added, way).wait_recv()

            def one(t, _):
                at = pl.multiple_of(t * chunk, chunk)
                value = part[pl.ds(pl.multiple_of(start + at, chunk), chunk), q * quarter : (q + 1) * quarter]
                if added is not None:
                    value = value + recv_buf[way, added, pl.ds(at, chunk), :].astype(jnp.float32)
                send_buf[way, k, pl.ds(at, chunk), :] = value.astype(jnp.bfloat16)
                return 0

            lax.fori_loop(0, 2, one, 0)
            message(tables, send_buf, recv_buf, sems, k, way).start()

    def close(tables, send_buf, recv_buf, sems, r, q, store):
        k = [tables[way].index((1, r, q)) for way in range(2)]
        for way in range(2):
            message(tables, send_buf, recv_buf, sems, k[way], way).wait_recv()
        start = z * block + r * rows

        def one(t, _):
            at = pl.multiple_of(t * chunk, chunk)
            value = part[pl.ds(pl.multiple_of(start + at, chunk), chunk), q * quarter : (q + 1) * quarter]
            for way in range(2):
                value = value + recv_buf[way, k[way], pl.ds(at, chunk), :].astype(jnp.float32)
            store(r, q, pl.ds(at, chunk), value)
            return 0

        lax.fori_loop(0, 2, one, 0)

    first_sum = (ONE, s_one, v_one, 0)
    second_sum = (TWO, s_two, v_two, 1)

    def gradient_part(g):
        token_finish(g)
        part[groups[g], :] = lax.dot_general(
            a_all[:, groups[g]], g_turned[...], (((0,), (0,)), ((), ())), preferred_element_type=jnp.float32
        )

    def keep_turned(r, q, at, value):
        turned[r, at, q * quarter : (q + 1) * quarter] = value.astype(jnp.bfloat16)

    def rotated_part(p, q):
        cols = slice(q * quarter, (q + 1) * quarter)
        part[pairs[p], cols] = jnp.dot(
            l_turn[pairs[p], :], turned[...].reshape(block, half)[:, cols], preferred_element_type=jnp.float32
        )

    def keep_rotated(r, q, at, value):
        rot_own[r, at, q * quarter : (q + 1) * quarter] = value

    for g, ready in ((1, (0, 1)), (2, ()), (3, (2, 3, 4, 5)), (4, ()), (5, (6, 7, 8)), (6, ()), (7, (9, 10)), (8, (11, 12))):
        gradient_part(g)
        for k in ready:
            send(*first_sum, k)
    for r in range(2):
        close(*first_sum, r, 0, keep_turned)
    send(*first_sum, 13)
    rotated_part(0, 0)
    send(*second_sum, 0)
    rotated_part(1, 0)
    send(*second_sum, 1)
    rotated_part(2, 0)
    rotated_part(3, 0)
    for r in range(2):
        close(*first_sum, r, 1, keep_turned)
    rotated_part(0, 1)
    send(*second_sum, 2)
    rotated_part(1, 1)
    send(*second_sum, 3)
    rotated_part(2, 1)
    rotated_part(3, 1)
    for k in range(4, 13):
        send(*second_sum, k)

    rot_copy = remote(rot_own.at[other], rot_in, pair_send.at[1], pair_recv.at[1], partner)
    x_rows = [pl.ds(pl.multiple_of(z * block + r * rows, rows), rows) for r in range(2)]
    res_copies = [remote(res_send, x_all.at[x_rows[r], :], pair_send.at[2], pair_recv.at[2], partner) for r in range(2)]
    out_first = pltpu.make_async_copy(f_buf, first_out, out_sem.at[0])
    out_second = pltpu.make_async_copy(s_buf, second_out, out_sem.at[1])

    def gather_message(k, way):
        back, r, q = GATHER[way][k]
        owner = mod(z - back, NZ) if way == 0 else mod(z + back, NZ)
        here = x_all.at[
            pl.ds(pl.multiple_of(owner * block + r * rows, rows), rows), q * quarter : (q + 1) * quarter
        ]
        return remote(here, here, x_send.at[way, k], x_recv.at[way, k], (up, down)[way])

    def close_rotated(r):
        for q in range(2):
            close(*second_sum, r, q, keep_rotated)

        @pl.when(c != r)
        def _():
            rot_copy.start()

    def restore(r):
        @pl.when(c == r)
        def _():
            rot_copy.wait_recv()
            for h in range(2):
                cols = slice(h * half, (h + 1) * half)
                turned_back = rot_own[r] if h == r else rot_in[...]
                first = BETA_ONE * m1[:, cols] + (1.0 - BETA_ONE) * turned_back
                second = BETA_TWO * m2[:, cols] + (1.0 - BETA_TWO) * turned_back * turned_back
                f_buf[:, cols] = first
                s_buf[:, cols] = second
                d_buf[:, cols] = (first / (jnp.sqrt(second) + EPS_DIVIDE)).astype(jnp.bfloat16)

            def half_of(which):
                return lax.dot_general(
                    d_buf[...], r_all[which * half : (which + 1) * half, :],
                    (((1,), (1,)), ((), ())), preferred_element_type=jnp.float32,
                ).astype(jnp.bfloat16)

            res_send[...] = half_of(1 - r)
            res_copies[r].start()
            x_all[x_rows[r], :] = half_of(r)

        @pl.when(c != r)
        def _():
            res_copies[r].wait_recv()

        for k in (2 * r, 2 * r + 1):
            for way in range(2):
                gather_message(k, way).start()

    close_rotated(0)
    send(*second_sum, 13)
    restore(0)
    close_rotated(1)
    restore(1)
    out_first.start()
    out_second.start()

    def add_update(at, first=False):
        value = jnp.dot(l_all[:, at], x_all[at, :], preferred_element_type=jnp.float32)
        upd[...] = value if first else upd[...] + value

    def arrived(way, k):
        gather_message(k, way).wait_recv()

    for k in range(4, MESSAGES):
        for way in range(2):
            arrived(way, before(tuple((-b, r, q) for b, r, q in GATHER[way]), (-GATHER[way][k][0], *GATHER[way][k][1:])))
            gather_message(k, way).start()
        if k == 7:
            add_update(pairs[3], first=True)
        if k == 11:
            add_update(pairs[2])
    for way, rest_of in ((0, (10, 11)), (1, (8, 9))):
        for k in rest_of:
            arrived(way, k)
    add_update(pairs[1])
    add_update(groups[3])
    for way in range(2):
        for k in (12, 13):
            arrived(way, k)
    add_update(groups[1])

    squares = jnp.sum(upd[...] * upd[...])
    n_col[0] = jnp.broadcast_to(squares, n_col.shape[1:])
    theirs_l = pl.ds(pl.multiple_of(other * rows, rows), rows)
    upd_copy = remote(upd.at[theirs_l, :], upd_other, pair_send.at[3], pair_recv.at[3], partner)
    n_copies = [
        remote(n_col.at[0], n_col.at[1 + i], n_send.at[0, i], n_recv.at[0], device) for i, device in enumerate(column)
    ]
    for copy in n_copies:
        copy.start()
    upd_copy.start()
    remote(n_col.at[1:], n_col.at[1:], n_send.at[0, 0], n_recv.at[0], partner).wait_recv()
    total = jnp.zeros(n_col.shape[1:], jnp.float32)
    for d in range(NZ * NC):
        back_z = lax.rem(z - d // NC + NZ, NZ)
        back_c = lax.rem(c - d % NC + NC, NC)
        total = total + n_col[back_z * NC + back_c]
    n_exp[0] = total
    e_copies = [
        remote(n_exp.at[0], n_exp.at[1 + i], n_send.at[1, i], n_recv.at[1], device) for i, device in enumerate(plane)
    ]
    for copy in e_copies:
        copy.start()
    upd_copy.wait_recv()
    remote(n_exp.at[1:], n_exp.at[1:], n_send.at[1, 0], n_recv.at[1], partner).wait_recv()
    cells = float(width * hidden)
    own_norm = jnp.sqrt(total / cells + EPS_MEAN)
    norms = jnp.zeros_like(total)
    for e in range(NY * NX):
        norms = norms + jnp.sqrt(n_exp[e] / cells + EPS_MEAN)
    below = jnp.maximum(own_norm, norms / float(NY * NX))
    rms_out[0] = jnp.max(own_norm)
    below = below[0:1, 0:1]
    own_half = upd[mine_l, :]
    other_half = upd_other[...]
    low = jnp.where(c == 0, own_half, other_half)
    high = jnp.where(c == 0, other_half, own_half)
    delta_out[:, :half] = (-low / below).astype(jnp.bfloat16)
    delta_out[:, half:] = (-high / below).astype(jnp.bfloat16)

    for g in range(len(groups) - 3, len(groups)):
        token_wait(g).wait_send()
    for copy in forwards + [l_copy, rot_copy, res_copies[0], upd_copy] + n_copies + e_copies:
        copy.wait_send()
    for k in range(MESSAGES):
        for way in range(2):
            message(*first_sum, k, way).wait_send()
            message(*second_sum, k, way).wait_send()
            gather_message(k, way).wait_send()
    out_first.wait()
    out_second.wait()


def local(acts, grad_out, routing_counts, left_basis, right_basis, first_moment, second_moment):
    width, hidden = acts.shape[-1], grad_out.shape[-1]
    rows = left_basis.shape[1]
    block, half = 2 * rows, hidden // 2
    quarter = half // 2
    own_tokens = acts.shape[1] * acts.shape[2]
    both = 2 * own_tokens
    bf16, f32 = jnp.bfloat16, jnp.float32
    vmem, dma = pltpu.VMEM, pltpu.SemaphoreType.DMA
    hbm = pl.BlockSpec(memory_space=pltpu.HBM)
    anywhere = pl.BlockSpec(memory_space=pl.ANY)
    scalars = pl.BlockSpec(memory_space=pltpu.SMEM)
    whole = pl.BlockSpec(memory_space=pltpu.VMEM)
    delta, first, second, rms = pl.pallas_call(
        kernel,
        name="soap_step",
        out_shape=(
            jax.ShapeDtypeStruct((rows, hidden), bf16),
            jax.ShapeDtypeStruct((rows, hidden), f32),
            jax.ShapeDtypeStruct((rows, hidden), f32),
            jax.ShapeDtypeStruct((1,), f32),
        ),
        in_specs=[hbm] * 7,
        out_specs=(whole, anywhere, anywhere, scalars),
        scratch_shapes=[
            pltpu.SMEM((1, NY * NX), jnp.int32),
            vmem((both, width), bf16),
            vmem((own_tokens, hidden), bf16),
            vmem((both, hidden), bf16),
            vmem((block, width), bf16),
            vmem((width, block), bf16),
            vmem((hidden, hidden), bf16),
            vmem((rows, hidden), f32),
            vmem((rows, hidden), f32),
            vmem((both, half), bf16),
            vmem((width, half), f32),
            vmem((2, MESSAGES, rows, quarter), bf16),
            vmem((2, MESSAGES, rows, quarter), bf16),
            vmem((2, MESSAGES, rows, quarter), bf16),
            vmem((2, MESSAGES, rows, quarter), bf16),
            vmem((2, rows, half), bf16),
            vmem((2, rows, half), f32),
            vmem((rows, half), f32),
            vmem((rows, half), bf16),
            vmem((width, half), bf16),
            vmem((block, half), f32),
            vmem((rows, half), f32),
            vmem((rows, hidden), bf16),
            vmem((rows, hidden), f32),
            vmem((rows, hidden), f32),
            vmem((NZ * NC, 8, 128), f32),
            vmem((NY * NX, 8, 128), f32),
            dma((7,)),
            dma((9,)), dma((9,)), dma((9,)), dma((9,)),
            dma((4,)), dma((4,)),
            dma((2, 2, MESSAGES)), dma((2, 2, MESSAGES)),
            dma((2, MESSAGES)), dma((2, MESSAGES)),
            dma((2, 15)), dma((2,)),
            dma((2,)),
        ],
        compiler_params=pltpu.CompilerParams(
            collective_id=0, has_side_effects=True, vmem_limit_bytes=52 * 1024 * 1024
        ),
    )(
        routing_counts,
        acts.reshape(own_tokens, width),
        grad_out.reshape(own_tokens, hidden),
        left_basis[0],
        right_basis[0],
        first_moment[0],
        second_moment[0],
    )
    return delta[None], first[None], second[None], rms


def solution(mesh):
    split = Mesh(mesh.devices.reshape(NY, NX, NZ, NC), AXES)
    placed = (
        P(AXES, None, None, None),
        P(AXES, None, None, None),
        P(AXES, None),
        P(EXPERT, DP, None),
        P(EXPERT, None, None),
        P(EXPERT, DP, None),
        P(EXPERT, DP, None),
    )
    return jax.shard_map(
        local,
        mesh=split,
        in_specs=placed,
        out_specs=(P(EXPERT, DP, None), P(EXPERT, DP, None), P(EXPERT, DP, None), P(EXPERT)),
        check_vma=False,
    )
```

```python
import functools

import jax
import jax.numpy as jnp
from jax import lax
from jax.experimental import pallas as pl
from jax.experimental.pallas import tpu as pltpu
from jax.sharding import Mesh
from jax.sharding import PartitionSpec as P

AXES = ("y", "x", "z", "core")
EXPERT = ("y", "x")
DP = ("z", "core")
NY, NX, NZ, NC = 4, 4, 8, 2
MESH = pl.DeviceIdType.MESH

BETA_ONE = 0.9
BETA_TWO = 0.95
EPS_DIVIDE = 1e-08
EPS_MEAN = 1e-06

PLANE = (
    (0, 1), (3, 0), (2, 2), (0, 3), (1, 0), (1, 2), (3, 2), (1, 1),
    (3, 3), (2, 1), (2, 3), (1, 3), (3, 1), (0, 2), (2, 0),
)
COLUMN = tuple((dz, dc) for dz in range(NZ) for dc in range(NC) if dz or dc)
ONE_UP = (
    (4, 0, 0), (4, 1, 1), (3, 1, 0), (3, 0, 1), (3, 0, 0), (3, 1, 1), (2, 1, 0),
    (2, 0, 0), (2, 0, 1), (1, 1, 0), (1, 0, 0), (2, 1, 1), (1, 0, 1), (1, 1, 1),
)
ONE = (ONE_UP, tuple((away, 1 - r, q) for away, r, q in ONE_UP))
TWO = (
    (
        (4, 0, 0), (3, 1, 0), (4, 1, 1), (3, 0, 1), (3, 0, 0), (2, 1, 0), (3, 1, 1),
        (2, 0, 1), (2, 0, 0), (1, 0, 1), (1, 0, 0), (2, 1, 1), (1, 1, 0), (1, 1, 1),
    ),
    (
        (4, 1, 0), (3, 0, 0), (4, 0, 1), (3, 1, 1), (3, 1, 0), (2, 0, 0), (3, 0, 1),
        (2, 1, 1), (2, 0, 1), (1, 0, 0), (1, 0, 1), (2, 1, 0), (1, 1, 1), (1, 1, 0),
    ),
)
NEAR = tuple((back, r, q) for back in range(3) for r in range(2) for q in range(2))
GATHER = (NEAR + ((3, 0, 0), (3, 0, 1)), NEAR + ((3, 1, 0), (3, 1, 1)))
MESSAGES = len(ONE_UP)


def before(table, message):
    away, r, q = message
    return {m: k for k, m in enumerate(table)}.get((away + 1, r, q))


def kernel(
    counts_in, acts, grads, left, right, first_in, second_in,
    delta_out, first_out, second_out, rms_out,
    counts, a_all, g_own, g_all, l_all, l_turn, r_all, m1, m2, g_turned, part, s_one, v_one, s_two, v_two,
    turned, rot_own, rot_in, res_send, x_all, upd, upd_other, d_buf, f_buf, s_buf, n_col, n_exp,
    load_sem, t_send, t_recv, fwd_send, fwd_recv, pair_send, pair_recv,
    r_send, r_recv, x_send, x_recv, n_send, n_recv, out_sem,
):
    y, x, z, c = (lax.axis_index(a) for a in AXES)
    other = 1 - c
    rows = left.shape[0]
    block = 2 * rows
    width = left.shape[1]
    hidden = grads.shape[1]
    half = hidden // 2
    quarter = half // 2
    slots = acts.shape[0] // (NY * NX)
    tokens = NY * NX * slots
    pair_wide = 2 * block

    def mod(v, n):
        return lax.rem(v + n, n)

    partner = (y, x, z, other)
    plane = [(mod(y + dy, NY), mod(x + dx, NX), z, c) for dy, dx in PLANE]
    column = [(y, x, mod(z + dz, NZ), mod(c + dc, NC)) for dz, dc in COLUMN]
    up = (y, x, mod(z + 1, NZ), c)
    down = (y, x, mod(z - 1, NZ), c)

    def remote(src, dst, send, recv, device):
        return pltpu.make_async_remote_copy(
            src_ref=src, dst_ref=dst, send_sem=send, recv_sem=recv, device_id=device, device_id_type=MESH
        )

    barrier = pltpu.get_barrier_semaphore()
    for device in plane + column:
        pl.semaphore_signal(barrier, 1, device_id=device, device_id_type=MESH)

    own_expert = y * NX + x
    mine_l = pl.ds(pl.multiple_of(c * rows, rows), rows)
    load_c = pltpu.make_async_copy(counts_in, counts, load_sem.at[6])
    load_g = pltpu.make_async_copy(grads, g_own, load_sem.at[0])
    load_a = pltpu.make_async_copy(
        acts.at[pl.ds(pl.multiple_of(own_expert * slots, slots), slots), :],
        a_all.at[pl.ds(pl.multiple_of(c * tokens, tokens), slots), :],
        load_sem.at[1],
    )
    load_l = pltpu.make_async_copy(left, l_all.at[mine_l, :], load_sem.at[2])
    load_r = pltpu.make_async_copy(right, r_all, load_sem.at[3])
    load_m1 = pltpu.make_async_copy(first_in, m1, load_sem.at[4])
    load_m2 = pltpu.make_async_copy(second_in, m2, load_sem.at[5])
    load_c.start()
    load_g.start()
    load_l.start()
    load_c.wait()
    load_g.wait()
    for load in (load_a, load_r, load_m1, load_m2):
        load.start()
    slot_index = lax.broadcasted_iota(jnp.int32, (slots, hidden), 0)
    for e in range(NY * NX):
        here = slice(e * slots, (e + 1) * slots)
        g_own[here, :] = jnp.where(slot_index < counts[0, e], g_own[here, :].astype(jnp.float32), 0.0).astype(jnp.bfloat16)
    pl.semaphore_wait(barrier, len(plane) + len(column))

    odd = lax.rem(z, 2)
    pair_of = [
        lax.rem(z // 2 + i, NZ // 2) * pair_wide for i in (2, 1 + 2 * odd, 3 - 2 * odd, 0)
    ]
    pairs = [pl.ds(pl.multiple_of(at, pair_wide), pair_wide) for at in pair_of]
    wide, rest = pair_wide * 4 // 7, pair_wide * 3 // 7

    def window(at, size):
        return pl.ds(pl.multiple_of(at, pair_wide // 7), size)

    groups = [None]
    for one, two in ((0, 1), (2, 3)):
        groups += [
            window(pair_of[one] + rest * odd, wide),
            window(pair_of[two] + rest * (1 - odd), wide),
            window(pair_of[one] + wide * (1 - odd), rest),
            window(pair_of[two] + wide * odd, rest),
        ]

    def token_rows(core, i):
        return pl.ds(pl.multiple_of(core * tokens + i * slots, slots), slots)

    t_copies = []
    for g, cols in enumerate(groups):
        copies = []
        for i, device in enumerate(plane):
            expert = device[0] * NX + device[1]
            src = pl.ds(pl.multiple_of(expert * slots, slots), slots)
            dst = token_rows(c, i + 1)
            if g == 0:
                ends = g_own.at[src, :], g_all.at[dst, :]
            else:
                ends = acts.at[src, cols], a_all.at[dst, cols]
            copies.append(remote(*ends, t_send.at[g], t_recv.at[g], device))
        t_copies.append(copies)

    def token_start(g):
        for copy in t_copies[g]:
            copy.start()

    def group_of(g, core, first, count):
        here = pl.ds(pl.multiple_of(core * tokens + first, slots), count)
        return g_all.at[here, :] if g == 0 else a_all.at[here, groups[g]]

    def token_wait(g):
        arrived = group_of(g, c, slots, tokens - slots)
        return remote(arrived, arrived, t_send.at[g], t_recv.at[g], partner)

    forwards = []
    for g in range(len(groups)):
        mine = group_of(g, c, 0, tokens)
        forwards.append(remote(mine, mine, fwd_send.at[g], fwd_recv.at[g], partner))

    def token_finish(g):
        token_wait(g).wait_recv()
        forwards[g].start()
        if g + 3 < len(groups):
            token_wait(g).wait_send()
            token_start(g + 3)
        theirs = group_of(g, other, 0, tokens)
        remote(theirs, theirs, fwd_send.at[g], fwd_recv.at[g], partner).wait_recv()

    for g in range(3):
        token_start(g)
    own_g = pl.ds(pl.multiple_of(own_expert * slots, slots), slots)
    g_all[token_rows(c, 0), :] = g_own[own_g, :]
    load_l.wait()
    l_copy = remote(l_all.at[mine_l, :], l_all.at[mine_l, :], pair_send.at[0], pair_recv.at[0], partner)
    l_copy.start()
    load_a.wait()
    load_r.wait()
    load_m1.wait()
    load_m2.wait()
    l_copy.wait_recv()
    for p in range(NZ // 2):
        at = slice(p * pair_wide, (p + 1) * pair_wide)
        l_turn[at, :] = l_all[:, at].T
    token_finish(0)
    g_turned[...] = jnp.dot(
        g_all[...], r_all[:, pl.ds(pl.multiple_of(c * half, half), half)], preferred_element_type=jnp.float32
    ).astype(jnp.bfloat16)

    chunk = rows // 2

    def message(tables, send_buf, recv_buf, sems, k, way):
        return remote(
            send_buf.at[way, k], recv_buf.at[way, k], r_send.at[sems, way, k], r_recv.at[sems, way, k], (up, down)[way]
        )

    def send(tables, send_buf, recv_buf, sems, k):
        for way in range(2):
            away, r, q = tables[way][k]
            owner = mod(z + away, NZ) if way == 0 else mod(z - away, NZ)
            start = owner * block + r * rows
            added = before(tables[way], tables[way][k])
            if added is not None:
                message(tables, send_buf, recv_buf, sems, added, way).wait_recv()

            def one(t, _):
                at = pl.multiple_of(t * chunk, chunk)
                value = part[pl.ds(pl.multiple_of(start + at, chunk), chunk), q * quarter : (q + 1) * quarter]
                if added is not None:
                    value = value + recv_buf[way, added, pl.ds(at, chunk), :].astype(jnp.float32)
                send_buf[way, k, pl.ds(at, chunk), :] = value.astype(jnp.bfloat16)
                return 0

            lax.fori_loop(0, 2, one, 0)
            message(tables, send_buf, recv_buf, sems, k, way).start()

    def close(tables, send_buf, recv_buf, sems, r, q, store):
        k = [tables[way].index((1, r, q)) for way in range(2)]
        for way in range(2):
            message(tables, send_buf, recv_buf, sems, k[way], way).wait_recv()
        start = z * block + r * rows

        def one(t, _):
            at = pl.multiple_of(t * chunk, chunk)
            value = part[pl.ds(pl.multiple_of(start + at, chunk), chunk), q * quarter : (q + 1) * quarter]
            for way in range(2):
                value = value + recv_buf[way, k[way], pl.ds(at, chunk), :].astype(jnp.float32)
            store(r, q, pl.ds(at, chunk), value)
            return 0

        lax.fori_loop(0, 2, one, 0)

    first_sum = (ONE, s_one, v_one, 0)
    second_sum = (TWO, s_two, v_two, 1)

    def gradient_part(g):
        token_finish(g)
        part[groups[g], :] = lax.dot_general(
            a_all[:, groups[g]], g_turned[...], (((0,), (0,)), ((), ())), preferred_element_type=jnp.float32
        )

    def keep_turned(r, q, at, value):
        turned[r, at, q * quarter : (q + 1) * quarter] = value.astype(jnp.bfloat16)

    def rotated_part(p, q):
        cols = slice(q * quarter, (q + 1) * quarter)
        part[pairs[p], cols] = jnp.dot(
            l_turn[pairs[p], :], turned[...].reshape(block, half)[:, cols], preferred_element_type=jnp.float32
        )

    def keep_rotated(r, q, at, value):
        rot_own[r, at, q * quarter : (q + 1) * quarter] = value

    for g, ready in ((1, (0, 1)), (2, ()), (3, (2, 3, 4, 5)), (4, ()), (5, (6, 7, 8)), (6, ()), (7, (9, 10)), (8, (11, 12))):
        gradient_part(g)
        for k in ready:
            send(*first_sum, k)
    for r in range(2):
        close(*first_sum, r, 0, keep_turned)
    send(*first_sum, 13)
    rotated_part(0, 0)
    send(*second_sum, 0)
    rotated_part(1, 0)
    send(*second_sum, 1)
    rotated_part(2, 0)
    rotated_part(3, 0)
    for r in range(2):
        close(*first_sum, r, 1, keep_turned)
    rotated_part(0, 1)
    send(*second_sum, 2)
    rotated_part(1, 1)
    send(*second_sum, 3)
    rotated_part(2, 1)
    rotated_part(3, 1)
    for k in range(4, 13):
        send(*second_sum, k)

    rot_copy = remote(rot_own.at[other], rot_in, pair_send.at[1], pair_recv.at[1], partner)
    x_rows = [pl.ds(pl.multiple_of(z * block + r * rows, rows), rows) for r in range(2)]
    res_copies = [remote(res_send, x_all.at[x_rows[r], :], pair_send.at[2], pair_recv.at[2], partner) for r in range(2)]
    out_first = pltpu.make_async_copy(f_buf, first_out, out_sem.at[0])
    out_second = pltpu.make_async_copy(s_buf, second_out, out_sem.at[1])

    def gather_message(k, way):
        back, r, q = GATHER[way][k]
        owner = mod(z - back, NZ) if way == 0 else mod(z + back, NZ)
        here = x_all.at[
            pl.ds(pl.multiple_of(owner * block + r * rows, rows), rows), q * quarter : (q + 1) * quarter
        ]
        return remote(here, here, x_send.at[way, k], x_recv.at[way, k], (up, down)[way])

    def close_rotated(r):
        for q in range(2):
            close(*second_sum, r, q, keep_rotated)

        @pl.when(c != r)
        def _():
            rot_copy.start()

    def restore(r):
        @pl.when(c == r)
        def _():
            rot_copy.wait_recv()
            for h in range(2):
                cols = slice(h * half, (h + 1) * half)
                turned_back = rot_own[r] if h == r else rot_in[...]
                first = BETA_ONE * m1[:, cols] + (1.0 - BETA_ONE) * turned_back
                second = BETA_TWO * m2[:, cols] + (1.0 - BETA_TWO) * turned_back * turned_back
                f_buf[:, cols] = first
                s_buf[:, cols] = second
                d_buf[:, cols] = (first / (jnp.sqrt(second) + EPS_DIVIDE)).astype(jnp.bfloat16)

            def half_of(which):
                return lax.dot_general(
                    d_buf[...], r_all[which * half : (which + 1) * half, :],
                    (((1,), (1,)), ((), ())), preferred_element_type=jnp.float32,
                ).astype(jnp.bfloat16)

            res_send[...] = half_of(1 - r)
            res_copies[r].start()
            x_all[x_rows[r], :] = half_of(r)

        @pl.when(c != r)
        def _():
            res_copies[r].wait_recv()

        for k in (2 * r, 2 * r + 1):
            for way in range(2):
                gather_message(k, way).start()

    close_rotated(0)
    send(*second_sum, 13)
    restore(0)
    close_rotated(1)
    restore(1)
    out_first.start()
    out_second.start()

    def add_update(at, first=False):
        value = jnp.dot(l_all[:, at], x_all[at, :], preferred_element_type=jnp.float32)
        upd[...] = value if first else upd[...] + value

    def arrived(way, k):
        gather_message(k, way).wait_recv()

    for k in range(4, MESSAGES):
        for way in range(2):
            arrived(way, before(tuple((-b, r, q) for b, r, q in GATHER[way]), (-GATHER[way][k][0], *GATHER[way][k][1:])))
            gather_message(k, way).start()
        if k == 7:
            add_update(pairs[3], first=True)
        if k == 11:
            add_update(pairs[2])
    for way, rest_of in ((0, (10, 11)), (1, (8, 9))):
        for k in rest_of:
            arrived(way, k)
    add_update(pairs[1])
    add_update(groups[3])
    for way in range(2):
        for k in (12, 13):
            arrived(way, k)
    add_update(groups[1])

    squares = jnp.sum(upd[...] * upd[...])
    n_col[0] = jnp.broadcast_to(squares, n_col.shape[1:])
    n_copies = [
        remote(n_col.at[0], n_col.at[1 + i], n_send.at[0, i], n_recv.at[0], device) for i, device in enumerate(column)
    ]
    for copy in n_copies:
        copy.start()
    theirs_l = pl.ds(pl.multiple_of(other * rows, rows), rows)
    upd_copy = remote(upd.at[theirs_l, :], upd_other, pair_send.at[3], pair_recv.at[3], partner)
    upd_copy.start()
    for g in range(len(groups) - 3, len(groups)):
        token_wait(g).wait_send()
    for copy in forwards + [l_copy, rot_copy, res_copies[0]]:
        copy.wait_send()
    for k in range(MESSAGES):
        for way in range(2):
            message(*first_sum, k, way).wait_send()
            message(*second_sum, k, way).wait_send()
            gather_message(k, way).wait_send()
    out_first.wait()
    out_second.wait()
    remote(n_col.at[1:], n_col.at[1:], n_send.at[0, 0], n_recv.at[0], partner).wait_recv()
    total = jnp.zeros(n_col.shape[1:], jnp.float32)
    for d in range(NZ * NC):
        back_z = lax.rem(z - d // NC + NZ, NZ)
        back_c = lax.rem(c - d % NC + NC, NC)
        total = total + n_col[back_z * NC + back_c]
    n_exp[0] = total
    e_copies = [
        remote(n_exp.at[0], n_exp.at[1 + i], n_send.at[1, i], n_recv.at[1], device) for i, device in enumerate(plane)
    ]
    for copy in e_copies:
        copy.start()
    cells = float(width * hidden)
    own_norm = jnp.sqrt(total / cells + EPS_MEAN)
    rms_out[0] = jnp.max(own_norm)
    upd_copy.wait_recv()
    own_half = upd[mine_l, :]
    other_half = upd_other[...]
    f_buf[:, :half] = jnp.where(c == 0, own_half, other_half)
    f_buf[:, half:] = jnp.where(c == 0, other_half, own_half)
    upd_copy.wait_send()
    for copy in n_copies:
        copy.wait_send()
    remote(n_exp.at[1:], n_exp.at[1:], n_send.at[1, 0], n_recv.at[1], partner).wait_recv()
    norms = jnp.zeros_like(total)
    for e in range(NY * NX):
        norms = norms + jnp.sqrt(n_exp[e] / cells + EPS_MEAN)
    scale = -1.0 / jnp.maximum(own_norm, norms / float(NY * NX))
    delta_out[...] = (f_buf[...] * scale[0:1, 0:1]).astype(jnp.bfloat16)
    for copy in e_copies:
        copy.wait_send()


def hand_on(*refs):
    count = (len(refs) - 1) // 3
    sources, results, held, sem = refs[:count], refs[count : 2 * count], refs[2 * count : 3 * count], refs[-1]
    loads = [pltpu.make_async_copy(a, v, sem.at[0, i]) for i, (a, v) in enumerate(zip(sources, held))]
    stores = [pltpu.make_async_copy(v, o, sem.at[1, i]) for i, (v, o) in enumerate(zip(held, results))]
    for load in loads:
        load.start()
    for load, store in zip(loads, stores):
        load.wait()
        store.start()
    for store in stores:
        store.wait()


def local(acts, grad_out, routing_counts, left_basis, right_basis, first_moment, second_moment):
    width, hidden = acts.shape[-1], grad_out.shape[-1]
    rows = left_basis.shape[1]
    block, half = 2 * rows, hidden // 2
    quarter = half // 2
    own_tokens = acts.shape[1] * acts.shape[2]
    both = 2 * own_tokens
    bf16, f32 = jnp.bfloat16, jnp.float32
    vmem, dma = pltpu.VMEM, pltpu.SemaphoreType.DMA
    hbm = pl.BlockSpec(memory_space=pltpu.HBM)
    anywhere = pl.BlockSpec(memory_space=pl.ANY)
    scalars = pl.BlockSpec(memory_space=pltpu.SMEM)
    whole = pl.BlockSpec(memory_space=pltpu.VMEM)
    delta, first, second, rms = pl.pallas_call(
        kernel,
        name="soap_step",
        out_shape=(
            jax.ShapeDtypeStruct((rows, hidden), bf16),
            jax.ShapeDtypeStruct((rows, hidden), f32),
            jax.ShapeDtypeStruct((rows, hidden), f32),
            jax.ShapeDtypeStruct((1,), f32),
        ),
        in_specs=[hbm] * 7,
        out_specs=(whole, anywhere, anywhere, scalars),
        scratch_shapes=[
            pltpu.SMEM((1, NY * NX), jnp.int32),
            vmem((both, width), bf16),
            vmem((own_tokens, hidden), bf16),
            vmem((both, hidden), bf16),
            vmem((block, width), bf16),
            vmem((width, block), bf16),
            vmem((hidden, hidden), bf16),
            vmem((rows, hidden), f32),
            vmem((rows, hidden), f32),
            vmem((both, half), bf16),
            vmem((width, half), f32),
            vmem((2, MESSAGES, rows, quarter), bf16),
            vmem((2, MESSAGES, rows, quarter), bf16),
            vmem((2, MESSAGES, rows, quarter), bf16),
            vmem((2, MESSAGES, rows, quarter), bf16),
            vmem((2, rows, half), bf16),
            vmem((2, rows, half), f32),
            vmem((rows, half), f32),
            vmem((rows, half), bf16),
            vmem((width, half), bf16),
            vmem((block, half), f32),
            vmem((rows, half), f32),
            vmem((rows, hidden), bf16),
            vmem((rows, hidden), f32),
            vmem((rows, hidden), f32),
            vmem((NZ * NC, 1, 128), f32),
            vmem((NY * NX, 1, 128), f32),
            dma((7,)),
            dma((9,)), dma((9,)), dma((9,)), dma((9,)),
            dma((4,)), dma((4,)),
            dma((2, 2, MESSAGES)), dma((2, 2, MESSAGES)),
            dma((2, MESSAGES)), dma((2, MESSAGES)),
            dma((2, 15)), dma((2,)),
            dma((2,)),
        ],
        compiler_params=pltpu.CompilerParams(
            collective_id=0, has_side_effects=True, vmem_limit_bytes=58000 * 1024
        ),
    )(
        routing_counts,
        acts.reshape(own_tokens, width),
        grad_out.reshape(own_tokens, hidden),
        left_basis[0],
        right_basis[0],
        first_moment[0],
        second_moment[0],
    )
    results = (second, first, delta)
    second, first, delta = pl.pallas_call(
        hand_on,
        name="hand_on",
        out_shape=tuple(jax.ShapeDtypeStruct(a.shape, a.dtype) for a in results),
        in_specs=[anywhere] * 3,
        out_specs=(anywhere,) * 3,
        scratch_shapes=[vmem(a.shape, a.dtype) for a in results] + [dma((2, 3))],
    )(*results)
    return delta[None], first[None], second[None], rms


def solution(mesh):
    split = Mesh(mesh.devices.reshape(NY, NX, NZ, NC), AXES)
    placed = (
        P(AXES, None, None, None),
        P(AXES, None, None, None),
        P(AXES, None),
        P(EXPERT, DP, None),
        P(EXPERT, None, None),
        P(EXPERT, DP, None),
        P(EXPERT, DP, None),
    )
    return jax.shard_map(
        local,
        mesh=split,
        in_specs=placed,
        out_specs=(P(EXPERT, DP, None), P(EXPERT, DP, None), P(EXPERT, DP, None), P(EXPERT)),
        check_vma=False,
    )
```
